32 devices in a mesh: freq: 2 (over x), param: 4 (over y, core), sens: 4 (over z).
Axes of the slice: x: 2, y: 2, z: 4, core: 2. Of those that a mesh axis runs over, the one named last changes fastest.
Arguments:
- series: bfloat16 [8, 600, 52], P(None, 'sens', 'freq'), may hold values from -6 to 6
- kernel: bfloat16 [2, 32, 600, 4096], P(None, 'freq', 'sens', 'param'), may hold values from -0.1875 to 0.1875
- prior_spectrum: float32 [32], P('freq'), may hold values from 0.3 to 1.5
- prior_scale: float32 [4096], P('param'), may hold values from 0.5 to 2
Outputs:
- adjoint_map: float32 [52, 8, 4096], P('freq', 'sens', 'param')
The draws below stay inside these ranges and needn't reach their ends.
All inputs are finite; a program needn't handle non-finite values.
Results may differ from the reference program's by a relative error of at most 0.0047.
Values may be sent and summed in bfloat16 or wider, within the bound.
No kernel may reach another device: no remote copies, remote signals or barrier semaphores. Data moves between devices by JAX's collectives and lax.ppermute only.
A program may use at most 64 MiB of HBM per device.

```python
import math
import jax
import jax.numpy as jnp
from jax import lax

SENSORS = 600
LEN = 840
NB = 32
NT = 52
NP = 4096
PROBES = 8


def level_of(rng, extent, pieces, smallest, high):
    def one(position, blocks):
        steps = jax.random.uniform(jax.random.fold_in(jax.random.fold_in(rng, 6), position), (blocks,), jnp.float32, smallest / len(pieces), high / len(pieces))
        return jnp.repeat(jnp.exp(steps), extent[position] // blocks).reshape((-1,) + (1,) * (len(extent) - position - 1))

    level = one(*pieces[0])
    for cut in pieces[1:]:
        level = level * one(*cut)
    return level


def noise(rng, extent, width, reach, cuts=(), kind=jnp.bfloat16):
    entries = jax.random.normal(rng, extent, jnp.float32) * width
    if len(cuts) > 0:
        entries = level_of(rng, extent, cuts, -0.22, 0.18) * entries
    return jnp.clip(entries, min=-reach, max=reach).astype(kind)


def setup_inputs(seed: int = 0) -> dict:
    key_of = jax.random.split(jax.random.key(seed), 5)
    series = noise(key_of[0], (PROBES, SENSORS, NT), 1.0, 6.0, ((1, 4), (2, 2)))
    kernel = noise(key_of[1], (2, NB, SENSORS, NP), (2 * SENSORS) ** -0.5, 0.1875, ((1, 2), (2, 4), (3, 4)))
    prior_spectrum = jnp.clip(jnp.exp(math.log(1.5) - 1.60943787 * jax.random.uniform(key_of[2], (NB,), jnp.float32) ** level_of(key_of[2], (NB,), ((0, 2),), -0.2, 0.2)), 0.3, 1.5)
    prior_scale = jnp.clip(jnp.exp(math.log(2.0) - 1.3862944 * jax.random.uniform(key_of[3], (NP,), jnp.float32) ** level_of(key_of[3], (NP,), ((0, 4),), -0.2, 0.2)), 0.5, 2.0)
    return {"series": series, "kernel": kernel, "prior_spectrum": prior_spectrum, "prior_scale": prior_scale}


def phase_tables(bin_count, time_count):
    bin_index = jnp.arange(bin_count, dtype=jnp.int32)
    time_index = jnp.arange(time_count, dtype=jnp.int32)
    product = time_index[:, None] * bin_index[None, :] % LEN
    phase_angle = product.astype(jnp.float32) * (2.0 * math.pi / LEN)
    return (jnp.cos(phase_angle), jnp.sin(phase_angle))

def reference(series, kernel, prior_spectrum, prior_scale):
    highest = lax.Precision.HIGHEST
    cosine, sine_part = phase_tables(NB, NT)
    flat_rows = series.astype(jnp.float32).reshape(PROBES * SENSORS, NT)
    norm_time = 1.0 / math.sqrt(NT)
    spec_re = (jnp.dot(flat_rows, cosine, precision=highest) * norm_time).astype(jnp.bfloat16)
    spec_im = (-jnp.dot(flat_rows, sine_part, precision=highest) * norm_time).astype(jnp.bfloat16)
    spec_re = spec_re.reshape(PROBES, SENSORS, NB).transpose(2, 1, 0)
    spec_im = spec_im.reshape(PROBES, SENSORS, NB).transpose(2, 1, 0)

    def one_bin(index):
        kern_re = kernel[0, index]
        kern_im = kernel[1, index]
        data_re = spec_re[index].T
        data_im = spec_im[index].T
        real_part = jnp.dot(data_re, kern_re, preferred_element_type=jnp.float32) + jnp.dot(data_im, kern_im, preferred_element_type=jnp.float32)
        imag_part = jnp.dot(data_im, kern_re, preferred_element_type=jnp.float32) - jnp.dot(data_re, kern_im, preferred_element_type=jnp.float32)
        return jnp.stack([real_part, imag_part])
    spectra = lax.map(one_bin, jnp.arange(NB, dtype=jnp.int32))
    weights = prior_spectrum / math.sqrt(NB)
    scaled_spec = spectra * weights[:, None, None, None]
    image_re = scaled_spec[:, 0].reshape(NB, PROBES * NP)
    image_im = scaled_spec[:, 1].reshape(NB, PROBES * NP)
    image_field = jnp.dot(cosine, image_re, precision=highest) - jnp.dot(sine_part, image_im, precision=highest)
    image_field = image_field.reshape(NT, PROBES, NP)
    weighted = image_field * prior_scale
    padded = jnp.pad(weighted, ((0, 0), (0, 0), (1, 1)))
    smooth = 0.5 * weighted + 0.25 * (padded[:, :, :-2] + padded[:, :, 2:])
    return smooth * prior_scale
```

```python
import functools
import math

import jax
import jax.numpy as jnp
from jax import lax
from jax.experimental import pallas as pl
from jax.experimental.pallas import tpu as pltpu
from jax.sharding import PartitionSpec as P

LEN = 840
BF = jnp.bfloat16
F32 = jnp.float32


def vmem():
    return pl.BlockSpec(memory_space=pltpu.VMEM)


def call(body, name, out_shape, *args, limit=40 << 20):
    return pl.pallas_call(
        body,
        in_specs=[vmem()] * len(args),
        out_specs=jax.tree.map(lambda _: vmem(), out_shape),
        out_shape=out_shape,
        compiler_params=pltpu.CompilerParams(vmem_limit_bytes=limit),
        name=name,
    )(*args)


def wave(product, part):
    angle = ((product + part * (LEN // 4)) % LEN).astype(F32) * (2.0 * math.pi / LEN)
    return jnp.cos(angle)


def split_index(flat, sizes):
    out = []
    for size in reversed(sizes):
        out.append(flat % size)
        flat = flat // size
    return out[::-1]


def iota(shape, dim):
    return lax.broadcasted_iota(jnp.int32, shape, dim)


def forward_table(piece, bins, times, probes, group):
    freq, sens = lax.axis_index("freq"), lax.axis_index("sens")
    freqs, senss = lax.axis_size("freq"), lax.axis_size("sens")
    shape = (senss * 2 * bins * group, times * probes)
    shift, part, bin_at, inner = split_index(iota(shape, 0), (senss, 2, bins, group))
    time, probe = split_index(iota(shape, 1), (times, probes))
    time = time + (freq + piece) % freqs * times
    hit = probe == (sens + shift) % senss * group + inner
    value = wave((freq * bins + bin_at) * time, part) * (1.0 / math.sqrt(times * freqs))
    return jnp.where(hit, value, 0.0)


def inverse_table(weights, bins, times, group, rows):
    freq, freqs = lax.axis_index("freq"), lax.axis_size("freq")
    shape = (freqs * rows, 2 * bins * group)
    shift, row = split_index(iota(shape, 0), (freqs, rows))
    time, outer = split_index(row, (times + 1, group))
    part, bin_at, inner = split_index(iota(shape, 1), (2, bins, group))
    hit = (outer == inner) & (row < times * group)
    time = time + (freq + shift) % freqs * times
    value = wave((freq * bins + bin_at) * time, part)
    weight = jnp.broadcast_to(weights[None, :, None], (2, bins, group)).reshape(1, -1)
    return jnp.where(hit, value * weight, 0.0)


def contract_body(bins, blocks, pieces, *refs):
    tables = refs[: 2 * pieces]
    series = refs[2 * pieces : 3 * pieces]
    spread, operator = refs[3 * pieces : 3 * pieces + 2]
    outs = refs[3 * pieces + 2 :]
    spec = None
    for i in range(2 * pieces):
        term = jnp.dot(tables[i][...], series[i // 2][...], preferred_element_type=F32)
        spec = term if spec is None else spec + term
    rows = spec.shape[0]
    inner = operator.shape[0] // 2
    block = rows // blocks
    half = block // 2
    group = half // bins
    wide = jnp.dot(spec.astype(BF), spread[...], preferred_element_type=F32)
    keep = iota(wide.shape, 0) // group % bins == iota(wide.shape, 1) % bins
    wide = jnp.where(keep, wide, 0.0).astype(BF)
    turned = []
    for i in range(blocks):
        turned += [wide[i * block + half : (i + 1) * block], -wide[i * block : i * block + half]]
    total = jnp.dot(wide, operator[:inner], preferred_element_type=F32)
    total = total + jnp.dot(
        jnp.concatenate(turned, axis=0), operator[inner:], preferred_element_type=F32
    )
    for i, out in enumerate(outs):
        out[...] = total[i * block : (i + 1) * block].astype(out.dtype)


def image_body(rows, *refs):
    table, own = refs[:2]
    count = table.shape[0] // rows
    outs = refs[len(refs) - count :]
    total = own[...]
    for other in refs[2 : len(refs) - count]:
        total = total + other[...].astype(F32)
    image = jnp.dot(
        table[...], total, precision=lax.Precision.HIGHEST, preferred_element_type=F32
    )
    for i, out in enumerate(outs):
        out[...] = image[i * rows : (i + 1) * rows].astype(out.dtype)


def rotate(value, axis, shift):
    size = lax.axis_size(axis)
    return lax.ppermute(value, axis, [(i, (i + shift) % size) for i in range(size)])


def local(series, kernel, prior_spectrum, prior_scale):
    freqs, senss, params = (lax.axis_size(a) for a in ("freq", "sens", "param"))
    probes, sens_dev, times = series.shape
    bins, cols = kernel.shape[1], kernel.shape[3]
    group = probes // senss
    block = 2 * bins * group
    own_series = series.transpose(2, 0, 1).reshape(times * probes, sens_dev)
    pieces = [own_series] + [rotate(own_series, "freq", -j) for j in range(1, freqs)]
    tables = []
    for j in range(freqs):
        full = forward_table(j, bins, times, probes, group)
        high = lax.reduce_precision(full, 8, 7)
        tables += [high.astype(BF), (full - high).astype(BF)]
    operator = kernel.transpose(0, 2, 1, 3).reshape(2 * sens_dev * bins, cols)
    spread_shape = (sens_dev, sens_dev * bins)
    spread = (iota(spread_shape, 0) == iota(spread_shape, 1) // bins).astype(BF)
    partial = call(
        functools.partial(contract_body, bins, senss, freqs),
        "contract",
        [jax.ShapeDtypeStruct((block, cols), BF if i else F32) for i in range(senss)],
        *tables, *pieces, spread, operator,
    )
    order = sorted(range(1, senss), key=lambda d: -min(d, senss - d))
    arrived = [rotate(partial[d], "sens", d) for d in order]
    rows = -(-times * group // 8) * 8
    weights = prior_spectrum * (1.0 / math.sqrt(bins * freqs))
    image = call(
        functools.partial(image_body, rows),
        "image",
        [jax.ShapeDtypeStruct((rows, cols), BF if i else F32) for i in range(freqs)],
        inverse_table(weights, bins, times, group, rows), partial[0], *arrived,
    )
    total = image[0]
    for j in range(1, freqs):
        total = total + rotate(image[j], "freq", j).astype(F32)
    weighted = total[: times * group].reshape(times, group, cols) * prior_scale
    right = [(i, i + 1) for i in range(params - 1)]
    left = [(i + 1, i) for i in range(params - 1)]
    before = lax.ppermute(weighted[:, :, cols - 1 :], "param", right)
    after = lax.ppermute(weighted[:, :, :1], "param", left)
    padded = jnp.concatenate([before, weighted, after], axis=2)
    smooth = 0.5 * weighted + 0.25 * (padded[:, :, :-2] + padded[:, :, 2:])
    return smooth * prior_scale


def solution(mesh):
    placed = (P(None, "sens", "freq"), P(None, "freq", "sens", "param"), P("freq"), P("param"))
    return jax.shard_map(
        local, mesh=mesh, in_specs=placed, out_specs=P("freq", "sens", "param"), check_vma=False
    )
```

```python
import functools
import math

import jax
import jax.numpy as jnp
from jax import lax
from jax.experimental import pallas as pl
from jax.experimental.pallas import tpu as pltpu
from jax.sharding import PartitionSpec as P

LEN = 840
PREP = 10**10
BF = jnp.bfloat16
F32 = jnp.float32


def vmem():
    return pl.BlockSpec(memory_space=pltpu.VMEM)


def call(body, name, out_shape, *args, flops=0, limit=4 << 20):
    moved = sum(a.size * a.dtype.itemsize for a in [*args, *jax.tree.leaves(out_shape)])
    return pl.pallas_call(
        body,
        in_specs=[vmem()] * len(args),
        out_specs=jax.tree.map(lambda _: vmem(), out_shape),
        out_shape=out_shape,
        compiler_params=pltpu.CompilerParams(vmem_limit_bytes=limit),
        cost_estimate=pl.CostEstimate(flops=flops, transcendentals=0, bytes_accessed=moved),
        name=name,
    )(*args)


def split_index(flat, sizes):
    out = []
    for size in reversed(sizes):
        out.append(flat % size)
        flat = flat // size
    return out[::-1]


def iota(shape, dim):
    return lax.broadcasted_iota(jnp.int32, shape, dim)


def onehot(shape, hit):
    return jnp.where(hit, jnp.ones(shape, F32), jnp.zeros(shape, F32)).astype(BF)


def dot(a, b, precision=None):
    return jnp.dot(a, b, precision=precision, preferred_element_type=F32)


def wave(product, part):
    angle = ((product + part * (LEN // 4)) % LEN).astype(F32) * (2.0 * math.pi / LEN)
    return jnp.cos(angle)


def prepare_body(dims, weights, *refs):
    bins, times, probes, group, freqs, senss, rows = dims
    freq, sens = lax.axis_index("freq"), lax.axis_index("sens")
    tables, spread, inverse = refs[: 2 * freqs], refs[2 * freqs], refs[2 * freqs + 1]
    small = (2 * bins, times)
    part, bin_at = split_index(iota(small, 0), (2, bins))
    tall = (senss * 2 * bins * group, 2 * bins)
    up = onehot(tall, iota(tall, 0) // group % (2 * bins) == iota(tall, 1))
    flat = (times, times * probes)
    out = onehot(flat, iota(flat, 1) // probes == iota(flat, 0))
    full = (tall[0], flat[1])
    shift = iota(full, 0) // (2 * bins * group)
    probe = (sens + shift) % senss * group + iota(full, 0) % group
    hit = iota(full, 1) % probes == probe
    for j in range(freqs):
        time = iota(small, 1) + (freq + j) % freqs * times
        value = wave((freq * bins + bin_at) * time, part) * (1.0 / math.sqrt(times * freqs))
        high = value.astype(BF)
        low = (value - high.astype(F32)).astype(BF)
        for i, piece in enumerate((high, low)):
            wide = dot(dot(up, piece).astype(BF), out)
            tables[2 * j + i][...] = jnp.where(hit, wide, 0.0).astype(BF)
    spread[...] = onehot(spread.shape, iota(spread.shape, 1) // bins == iota(spread.shape, 0))
    shape = inverse.shape
    shift, row = split_index(iota(shape, 0), (freqs, rows))
    part, bin_at, inner = split_index(iota(shape, 1), (2, bins, group))
    time = row // group + (freq + shift) % freqs * times
    value = wave((freq * bins + bin_at) * time, part)
    pick = (bins, shape[1])
    chosen = jnp.where(iota(pick, 1) // group % bins == iota(pick, 0), 1.0, 0.0)
    weight = dot(weights[...], chosen, lax.Precision.HIGHEST) * (1.0 / math.sqrt(bins * freqs))
    hit = (row % group == inner) & (row < times * group)
    inverse[...] = jnp.where(hit, value * weight[:1], 0.0)


def contract_body(bins, blocks, pieces, *refs):
    tables = refs[: 2 * pieces]
    series = refs[2 * pieces : 3 * pieces]
    spread, operator = refs[3 * pieces : 3 * pieces + 2]
    lhs_re, lhs_im = refs[3 * pieces + 2 : 3 * pieces + 4]
    spec = None
    for i in range(2 * pieces):
        term = dot(tables[i][...], series[i // 2][...])
        spec = term if spec is None else spec + term
    rows = spec.shape[0]
    block = rows // blocks
    half = block // 2
    group = half // bins
    wide = dot(spec.astype(BF), spread[...])
    keep = iota(wide.shape, 0) // group % bins == iota(wide.shape, 1) % bins
    wide = jnp.where(keep, wide, 0.0).astype(BF)
    lhs_re[...] = wide
    for i in range(blocks):
        lhs_im[i * block : i * block + half, :] = wide[i * block + half : (i + 1) * block]
        lhs_im[i * block + half : (i + 1) * block, :] = -wide[i * block : i * block + half]
    outer_body(lhs_re, lhs_im, operator, *refs[3 * pieces + 4 :])


def product(lhs_re, lhs_im, operator, first, count):
    inner = operator.shape[0] // 2
    at = pl.ds(first, count)
    return dot(lhs_re[...], operator[:inner, at]) + dot(lhs_im[...], operator[inner:, at])


def outer_body(lhs_re, lhs_im, operator, *outs):
    cols = operator.shape[1]
    edge = cols // 4
    block = lhs_re.shape[0] // len(outs)
    for at, first in ((0, 0), (edge, cols - edge)):
        total = product(lhs_re, lhs_im, operator, first, edge)
        for i, out in enumerate(outs):
            out[:, at : at + edge] = total[i * block : (i + 1) * block].astype(out.dtype)


def inner_body(lhs_re, lhs_im, operator, *outs):
    cols = operator.shape[1]
    block = lhs_re.shape[0] // len(outs)
    total = product(lhs_re, lhs_im, operator, cols // 4, cols // 2)
    for i, out in enumerate(outs):
        out[...] = total[i * block : (i + 1) * block].astype(out.dtype)


def image_body(rows, *refs):
    table, own = refs[:2]
    count = table.shape[0] // rows
    outs = refs[len(refs) - count :]
    total = own[...]
    for other in refs[2 : len(refs) - count]:
        total = total + other[...].astype(F32)
    image = dot(table[...], total, lax.Precision.HIGHEST)
    for i, out in enumerate(outs):
        out[...] = image[i * rows : (i + 1) * rows].astype(out.dtype)


def edge_body(lanes, scale, *refs):
    first, last = refs[-2:]
    cols, width = scale.shape[1], refs[0].shape[1]
    for out, at, scale_at in ((first, 0, 0), (last, width - lanes, cols - lanes)):
        total = None
        for ref in refs[:-2]:
            term = ref[:, at : at + lanes].astype(F32)
            total = term if total is None else total + term
        out[...] = total * scale[:, scale_at : scale_at + lanes]


def smooth_body(count, scale, before, after, *refs):
    out = refs[-1]
    def total(parts):
        value = parts[0][...]
        for ref in parts[1:]:
            value = value + ref[...].astype(F32)
        return value
    outer, inner = total(refs[:count]), total(refs[count:-1])
    times, group, cols = out.shape
    edge = cols // 4
    value = jnp.concatenate([outer[:, :edge], inner, outer[:, edge:]], axis=1)
    value = value * scale[...]
    lane = iota(value.shape, 1)
    width = before.shape[1]
    left = jnp.where(lane == 0, before[:, width - 1 :], pltpu.roll(value, 1, 1))
    right = jnp.where(lane == cols - 1, after[:, :1], pltpu.roll(value, cols - 1, 1))
    value = (0.5 * value + 0.25 * (left + right)) * scale[...]
    out[...] = value[: times * group].reshape(times, group, cols)


def rotate(value, axis, shift):
    size = lax.axis_size(axis)
    return lax.ppermute(value, axis, [(i, (i + shift) % size) for i in range(size)])


def local(series, kernel, prior_spectrum, prior_scale):
    freqs, senss, params = (lax.axis_size(a) for a in ("freq", "sens", "param"))
    probes, sens_dev, times = series.shape
    bins, cols = kernel.shape[1], kernel.shape[3]
    group = probes // senss
    block = 2 * bins * group
    rows = -(-times * group // 8) * 8
    shape = jax.ShapeDtypeStruct
    own_series = series.transpose(2, 0, 1).reshape(times * probes, sens_dev)
    pieces = [own_series] + [rotate(own_series, "freq", -j) for j in range(1, freqs)]
    *tables, spread, inverse = call(
        functools.partial(prepare_body, (bins, times, probes, group, freqs, senss, rows)),
        "prepare",
        [shape((senss * block, times * probes), BF)] * (2 * freqs)
        + [shape((sens_dev, sens_dev * bins), BF), shape((freqs * rows, block), F32)],
        prior_spectrum.reshape(1, bins),
        flops=PREP,
    )
    operator = kernel.transpose(0, 2, 1, 3).reshape(2 * sens_dev * bins, cols)
    half = [shape((block, cols // 2), BF if i else F32) for i in range(senss)]
    lhs_re, lhs_im, *outer = call(
        functools.partial(contract_body, bins, senss, freqs),
        "contract_outer",
        [shape((senss * block, sens_dev * bins), BF)] * 2 + half,
        *tables, *pieces, spread, operator,
    )
    inner = call(inner_body, "contract_inner", half, lhs_re, lhs_im, operator)
    order = sorted(range(1, senss), key=lambda d: -min(d, senss - d))
    outer_parts = [outer[0]] + [rotate(outer[d], "sens", d) for d in order]
    inner_parts = [inner[0]] + [rotate(inner[d], "sens", d) for d in order]
    image = [shape((rows, cols // 2), BF if i else F32) for i in range(freqs)]
    as_image = functools.partial(image_body, rows)
    outer = call(as_image, "image_outer", image, inverse, *outer_parts)
    outer = [outer[0]] + [rotate(outer[j], "freq", j) for j in range(1, freqs)]
    inner = call(as_image, "image_inner", image, inverse, *inner_parts)
    inner = [inner[0]] + [rotate(inner[j], "freq", j) for j in range(1, freqs)]
    scale = prior_scale.reshape(1, cols)
    lanes = min(128, cols // 4)
    first, last = call(
        functools.partial(edge_body, lanes), "edge", [shape((rows, lanes), F32)] * 2, scale, *outer
    )
    before = lax.ppermute(last, "param", [(i, i + 1) for i in range(params - 1)])
    after = lax.ppermute(first, "param", [(i + 1, i) for i in range(params - 1)])
    return call(
        functools.partial(smooth_body, freqs),
        "smooth",
        shape((times, group, cols), F32),
        scale, before, after, *outer, *inner,
    )


def solution(mesh):
    placed = (P(None, "sens", "freq"), P(None, "freq", "sens", "param"), P("freq"), P("param"))
    return jax.shard_map(
        local, mesh=mesh, in_specs=placed, out_specs=P("freq", "sens", "param"), check_vma=False
    )
```

```python
import functools
import math

import jax
import jax.numpy as jnp
from jax import lax
from jax.experimental import pallas as pl
from jax.experimental.pallas import tpu as pltpu
from jax.sharding import PartitionSpec as P

LEN = 840
OUTER = 4
PREP = 10**10
BF = jnp.bfloat16
F32 = jnp.float32


def vmem():
    return pl.BlockSpec(memory_space=pltpu.VMEM)


def call(body, name, out_shape, *args, flops=0, limit=4 << 20):
    moved = sum(a.size * a.dtype.itemsize for a in [*args, *jax.tree.leaves(out_shape)])
    return pl.pallas_call(
        body,
        in_specs=[vmem()] * len(args),
        out_specs=jax.tree.map(lambda _: vmem(), out_shape),
        out_shape=out_shape,
        compiler_params=pltpu.CompilerParams(vmem_limit_bytes=limit),
        cost_estimate=pl.CostEstimate(flops=flops, transcendentals=0, bytes_accessed=moved),
        name=name,
    )(*args)


def split_index(flat, sizes):
    out = []
    for size in reversed(sizes):
        out.append(flat % size)
        flat = flat // size
    return out[::-1]


def iota(shape, dim):
    return lax.broadcasted_iota(jnp.int32, shape, dim)


def onehot(shape, hit):
    return jnp.where(hit, jnp.ones(shape, F32), jnp.zeros(shape, F32)).astype(BF)


def dot(a, b, precision=None):
    return jnp.dot(a, b, precision=precision, preferred_element_type=F32)


def wave(product, part):
    angle = ((product + part * (LEN // 4)) % LEN).astype(F32) * (2.0 * math.pi / LEN)
    return jnp.cos(angle)


def prepare_body(dims, *refs):
    bins, times, probes, group, freqs, senss = dims
    freq, sens = lax.axis_index("freq"), lax.axis_index("sens")
    tables, spread = refs[: 2 * freqs], refs[2 * freqs]
    small = (2 * bins, times)
    part, bin_at = split_index(iota(small, 0), (2, bins))
    tall = (senss * 2 * bins * group, 2 * bins)
    up = onehot(tall, iota(tall, 0) // group % (2 * bins) == iota(tall, 1))
    flat = (times, times * probes)
    out = onehot(flat, iota(flat, 1) // probes == iota(flat, 0))
    full = (tall[0], flat[1])
    shift = iota(full, 0) // (2 * bins * group)
    probe = (sens + shift) % senss * group + iota(full, 0) % group
    hit = iota(full, 1) % probes == probe
    for j in range(freqs):
        time = iota(small, 1) + (freq + j) % freqs * times
        value = wave((freq * bins + bin_at) * time, part) * (1.0 / math.sqrt(times * freqs))
        high = value.astype(BF)
        low = (value - high.astype(F32)).astype(BF)
        for i, piece in enumerate((high, low)):
            wide = dot(dot(up, piece).astype(BF), out)
            tables[2 * j + i][...] = jnp.where(hit, wide, 0.0).astype(BF)
    spread[...] = onehot(spread.shape, iota(spread.shape, 1) // bins == iota(spread.shape, 0))


def inverse_body(dims, weights, after, inverse):
    bins, times, group, freqs, rows = dims
    freq = lax.axis_index("freq")
    shape = inverse.shape
    shift, row = split_index(iota(shape, 0), (freqs, rows))
    part, bin_at, inner = split_index(iota(shape, 1), (2, bins, group))
    time = row // group + (freq + shift) % freqs * times
    value = wave((freq * bins + bin_at) * time, part)
    pick = (bins, shape[1])
    chosen = jnp.where(iota(pick, 1) // group % bins == iota(pick, 0), 1.0, 0.0)
    weight = dot(weights[...], chosen, lax.Precision.HIGHEST) * (1.0 / math.sqrt(bins * freqs))
    hit = (row % group == inner) & (row < times * group)
    inverse[...] = jnp.where(hit, value * weight[:1], 0.0)


def contract_body(bins, blocks, pieces, *refs):
    tables = refs[: 2 * pieces]
    series = refs[2 * pieces : 3 * pieces]
    spread, operator = refs[3 * pieces : 3 * pieces + 2]
    lhs_re, lhs_im = refs[3 * pieces + 2 : 3 * pieces + 4]
    spec = None
    for i in range(2 * pieces):
        term = dot(tables[i][...], series[i // 2][...])
        spec = term if spec is None else spec + term
    rows = spec.shape[0]
    block = rows // blocks
    half = block // 2
    group = half // bins
    wide = dot(spec.astype(BF), spread[...])
    keep = iota(wide.shape, 0) // group % bins == iota(wide.shape, 1) % bins
    wide = jnp.where(keep, wide, 0.0).astype(BF)
    lhs_re[...] = wide
    for i in range(blocks):
        lhs_im[i * block : i * block + half, :] = wide[i * block + half : (i + 1) * block]
        lhs_im[i * block + half : (i + 1) * block, :] = -wide[i * block : i * block + half]
    outer_body(lhs_re, lhs_im, operator, *refs[3 * pieces + 4 :])


def product(lhs_re, lhs_im, operator, first, count):
    inner = operator.shape[0] // 2
    at = pl.ds(first, count)
    return dot(lhs_re[...], operator[:inner, at]) + dot(lhs_im[...], operator[inner:, at])


def outer_body(lhs_re, lhs_im, operator, *outs):
    cols, edge = operator.shape[1], outs[0].shape[1] // 2
    block = lhs_re.shape[0] // len(outs)
    for at, first in ((0, 0), (edge, cols - edge)):
        total = product(lhs_re, lhs_im, operator, first, edge)
        for i, out in enumerate(outs):
            out[:, at : at + edge] = total[i * block : (i + 1) * block].astype(out.dtype)


def inner_body(lhs_re, lhs_im, operator, *outs):
    width = outs[0].shape[1]
    block = lhs_re.shape[0] // len(outs)
    total = product(lhs_re, lhs_im, operator, (operator.shape[1] - width) // 2, width)
    for i, out in enumerate(outs):
        out[...] = total[i * block : (i + 1) * block].astype(out.dtype)


def image_body(rows, *refs):
    table, own = refs[:2]
    count = table.shape[0] // rows
    outs = refs[len(refs) - count :]
    total = own[...]
    for other in refs[2 : len(refs) - count]:
        total = total + other[...].astype(F32)
    image = dot(table[...], total, lax.Precision.HIGHEST)
    for i, out in enumerate(outs):
        out[...] = image[i * rows : (i + 1) * rows].astype(out.dtype)


def edge_body(lanes, scale, *refs):
    within, across = refs[-2:]
    cols, width = scale.shape[1], refs[0].shape[1]

    def scaled(at, scale_at):
        total = None
        for ref in refs[:-2]:
            term = ref[:, at : at + lanes].astype(F32)
            total = term if total is None else total + term
        return total * scale[:, scale_at : scale_at + lanes]

    first, last = scaled(0, 0), scaled(width - lanes, cols - lanes)
    even = lax.axis_index("param") % 2 == 0
    within[...] = jnp.where(even, last, first)
    across[...] = jnp.where(even, first, last)


def smooth_body(count, scale, within, across, *refs):
    out = refs[-1]

    def total(parts):
        value = parts[0][...]
        for ref in parts[1:]:
            value = value + ref[...].astype(F32)
        return value

    outer, inner = total(refs[:count]), total(refs[count:-1])
    times, group, cols = out.shape
    edge = outer.shape[1] // 2
    value = jnp.concatenate([outer[:, :edge], inner, outer[:, edge:]], axis=1)
    value = value * scale[...]
    lane = iota(value.shape, 1)
    width = within.shape[1]
    even = lax.axis_index("param") % 2 == 0
    before = jnp.where(even, across[:, width - 1 :], within[:, width - 1 :])
    after = jnp.where(even, within[:, :1], across[:, :1])
    left = jnp.where(lane == 0, before, pltpu.roll(value, 1, 1))
    right = jnp.where(lane == cols - 1, after, pltpu.roll(value, cols - 1, 1))
    value = (0.5 * value + 0.25 * (left + right)) * scale[...]
    out[...] = value[: times * group].reshape(times, group, cols)


def rotate(value, axis, shift):
    size = lax.axis_size(axis)
    return lax.ppermute(value, axis, [(i, (i + shift) % size) for i in range(size)])


def local(series, kernel, prior_spectrum, prior_scale):
    freqs, senss, params = (lax.axis_size(a) for a in ("freq", "sens", "param"))
    probes, sens_dev, times = series.shape
    bins, cols = kernel.shape[1], kernel.shape[3]
    group = probes // senss
    block = 2 * bins * group
    rows = -(-times * group // 8) * 8
    shape = jax.ShapeDtypeStruct
    own_series = series.transpose(2, 0, 1).reshape(times * probes, sens_dev)
    pieces = [own_series] + [rotate(own_series, "freq", -j) for j in range(1, freqs)]
    *tables, spread = call(
        functools.partial(prepare_body, (bins, times, probes, group, freqs, senss)),
        "prepare",
        [shape((senss * block, times * probes), BF)] * (2 * freqs)
        + [shape((sens_dev, sens_dev * bins), BF)],
        flops=PREP,
    )
    operator = kernel.transpose(0, 2, 1, 3).reshape(2 * sens_dev * bins, cols)
    edge = cols // OUTER
    blocks = lambda width: [shape((block, width), BF if i else F32) for i in range(senss)]
    lhs_re, lhs_im, *outer = call(
        functools.partial(contract_body, bins, senss, freqs),
        "contract_outer",
        [shape((senss * block, sens_dev * bins), BF)] * 2 + blocks(2 * edge),
        *tables, *pieces, spread, operator,
    )
    inner = call(
        inner_body, "contract_inner", blocks(cols - 2 * edge), lhs_re, lhs_im, operator
    )
    inverse = call(
        functools.partial(inverse_body, (bins, times, group, freqs, rows)),
        "inverse",
        shape((freqs * rows, block), F32),
        prior_spectrum.reshape(1, bins), outer[0],
    )
    order = sorted(range(1, senss), key=lambda d: -min(d, senss - d))
    outer = [outer[0]] + [rotate(outer[d], "sens", d) for d in order]
    inner = [inner[0]] + [rotate(inner[d], "sens", d) for d in order]
    images = lambda width: [shape((rows, width), BF if i else F32) for i in range(freqs)]
    as_image = functools.partial(image_body, rows)
    outer = call(as_image, "image_outer", images(2 * edge), inverse, *outer)
    outer = [outer[0]] + [rotate(outer[j], "freq", j) for j in range(1, freqs)]
    inner = call(as_image, "image_inner", images(cols - 2 * edge), inverse, *inner)
    inner = [inner[0]] + [rotate(inner[j], "freq", j) for j in range(1, freqs)]
    scale = prior_scale.reshape(1, cols)
    lanes = min(128, edge)
    swaps = call(
        functools.partial(edge_body, lanes), "edge", [shape((rows, lanes), F32)] * 2, scale, *outer
    )
    swaps = [
        lax.ppermute(swaps[i], "param", [(a + d, a + 1 - d) for a in range(i, params - 1, 2) for d in (0, 1)])
        for i in (0, 1)
    ]
    return call(
        functools.partial(smooth_body, freqs),
        "smooth",
        shape((times, group, cols), F32),
        scale, *swaps, *outer, *inner,
    )


def solution(mesh):
    placed = (P(None, "sens", "freq"), P(None, "freq", "sens", "param"), P("freq"), P("param"))
    return jax.shard_map(
        local, mesh=mesh, in_specs=placed, out_specs=P("freq", "sens", "param"), check_vma=False
    )
```

```python
import functools
import math

import jax
import jax.numpy as jnp
from jax import lax
from jax.experimental import pallas as pl
from jax.experimental.pallas import tpu as pltpu
from jax.sharding import PartitionSpec as P


LEN = 840
OUTER = 4
PREP = 10**10
BF = jnp.bfloat16
F32 = jnp.float32


def vmem():
    return pl.BlockSpec(memory_space=pltpu.VMEM)


def call(body, out_shape, *args, flops=0, limit=4 << 20):
    moved = sum(a.size * a.dtype.itemsize for a in [*args, *jax.tree.leaves(out_shape)])
    return pl.pallas_call(
        body,
        in_specs=[vmem()] * len(args),
        out_specs=jax.tree.map(lambda _: vmem(), out_shape),
        out_shape=out_shape,
        compiler_params=pltpu.CompilerParams(vmem_limit_bytes=limit),
        cost_estimate=pl.CostEstimate(flops=flops, transcendentals=0, bytes_accessed=moved),
    )(*args)


def split_index(flat, sizes):
    out = []
    for size in reversed(sizes):
        out.append(flat % size)
        flat = flat // size
    return out[::-1]


def iota(shape, dim):
    return lax.broadcasted_iota(jnp.int32, shape, dim)


def onehot(shape, hit):
    return jnp.where(hit, jnp.ones(shape, F32), jnp.zeros(shape, F32)).astype(BF)


def dot(a, b, precision=None):
    return jnp.dot(a, b, precision=precision, preferred_element_type=F32)


def wave(product, part):
    angle = ((product + part * (LEN // 4)) % LEN).astype(F32) * (2.0 * math.pi / LEN)
    return jnp.cos(angle)


def prepare_body(dims, *refs):
    bins, times, probes, group, freqs, senss = dims
    freq, sens = lax.axis_index("freq"), lax.axis_index("sens")
    tables, spread = refs[: 2 * freqs], refs[2 * freqs]
    small = (2 * bins, times)
    part, bin_at = split_index(iota(small, 0), (2, bins))
    tall = (senss * 2 * bins * group, 2 * bins)
    up = onehot(tall, iota(tall, 0) // group % (2 * bins) == iota(tall, 1))
    flat = (times, times * probes)
    out = onehot(flat, iota(flat, 1) // probes == iota(flat, 0))
    full = (tall[0], flat[1])
    shift = iota(full, 0) // (2 * bins * group)
    probe = (sens + shift) % senss * group + iota(full, 0) % group
    hit = iota(full, 1) % probes == probe
    for j in range(freqs):
        time = iota(small, 1) + (freq + j) % freqs * times
        value = wave((freq * bins + bin_at) * time, part) * (1.0 / math.sqrt(times * freqs))
        high = value.astype(BF)
        low = (value - high.astype(F32)).astype(BF)
        for i, piece in enumerate((high, low)):
            wide = dot(dot(up, piece).astype(BF), out)
            tables[2 * j + i][...] = jnp.where(hit, wide, 0.0).astype(BF)
    spread[...] = onehot(spread.shape, iota(spread.shape, 1) // bins == iota(spread.shape, 0))


def inverse_body(dims, weights, after, inverse):
    bins, times, group, freqs, rows = dims
    freq = lax.axis_index("freq")
    shape = inverse.shape
    shift, row = split_index(iota(shape, 0), (freqs, rows))
    part, bin_at, inner = split_index(iota(shape, 1), (2, bins, group))
    time = row // group + (freq + shift) % freqs * times
    value = wave((freq * bins + bin_at) * time, part)
    pick = (bins, shape[1])
    chosen = jnp.where(iota(pick, 1) // group % bins == iota(pick, 0), 1.0, 0.0)
    weight = dot(weights[...], chosen, lax.Precision.HIGHEST) * (1.0 / math.sqrt(bins * freqs))
    hit = (row % group == inner) & (row < times * group)
    inverse[...] = jnp.where(hit, value * weight[:1], 0.0)


def contract_body(bins, blocks, pieces, *refs):
    tables = refs[: 2 * pieces]
    series = refs[2 * pieces : 3 * pieces]
    spread, operator = refs[3 * pieces : 3 * pieces + 2]
    lhs_re, lhs_im = refs[3 * pieces + 2 : 3 * pieces + 4]
    spec = None
    for i in range(2 * pieces):
        term = dot(tables[i][...], series[i // 2][...])
        spec = term if spec is None else spec + term
    rows = spec.shape[0]
    block = rows // blocks
    half = block // 2
    group = half // bins
    wide = dot(spec.astype(BF), spread[...])
    keep = iota(wide.shape, 0) // group % bins == iota(wide.shape, 1) % bins
    wide = jnp.where(keep, wide, 0.0).astype(BF)
    lhs_re[...] = wide
    for i in range(blocks):
        lhs_im[i * block : i * block + half, :] = wide[i * block + half : (i + 1) * block]
        lhs_im[i * block + half : (i + 1) * block, :] = -wide[i * block : i * block + half]
    outer_body(lhs_re, lhs_im, operator, *refs[3 * pieces + 4 :])


def product(lhs_re, lhs_im, operator, first, count):
    inner = operator.shape[0] // 2
    at = pl.ds(first, count)
    return dot(lhs_re[...], operator[:inner, at]) + dot(lhs_im[...], operator[inner:, at])


def outer_body(lhs_re, lhs_im, operator, *outs):
    cols, edge = operator.shape[1], outs[0].shape[1] // 2
    block = lhs_re.shape[0] // len(outs)
    for at, first in ((0, 0), (edge, cols - edge)):
        total = product(lhs_re, lhs_im, operator, first, edge)
        for i, out in enumerate(outs):
            out[:, at : at + edge] = total[i * block : (i + 1) * block].astype(out.dtype)


def inner_body(lhs_re, lhs_im, operator, *outs):
    width = outs[0].shape[1]
    block = lhs_re.shape[0] // len(outs)
    total = product(lhs_re, lhs_im, operator, (operator.shape[1] - width) // 2, width)
    for i, out in enumerate(outs):
        out[...] = total[i * block : (i + 1) * block].astype(out.dtype)


def image_body(rows, *refs):
    table, own = refs[:2]
    count = table.shape[0] // rows
    outs = refs[len(refs) - count :]
    total = own[...]
    for other in refs[2 : len(refs) - count]:
        total = total + other[...].astype(F32)
    image = dot(table[...], total, lax.Precision.HIGHEST)
    for i, out in enumerate(outs):
        out[...] = image[i * rows : (i + 1) * rows].astype(out.dtype)


def edge_body(lanes, scale, *refs):
    within, across = refs[-2:]
    cols, width = scale.shape[1], refs[0].shape[1]

    def scaled(at, scale_at):
        total = None
        for ref in refs[:-2]:
            term = ref[:, at : at + lanes].astype(F32)
            total = term if total is None else total + term
        return total * scale[:, scale_at : scale_at + lanes]

    first, last = scaled(0, 0), scaled(width - lanes, cols - lanes)
    even = lax.axis_index("param") % 2 == 0
    within[...] = jnp.where(even, last, first)
    across[...] = jnp.where(even, first, last)


def smooth_body(count, scale, within, across, *refs):
    out = refs[-1]

    def total(parts):
        value = parts[0][...]
        for ref in parts[1:]:
            value = value + ref[...].astype(F32)
        return value

    outer, inner = total(refs[:count]), total(refs[count:-1])
    times, group, cols = out.shape
    edge = outer.shape[1] // 2
    value = jnp.concatenate([outer[:, :edge], inner, outer[:, edge:]], axis=1)
    value = value * scale[...]
    lane = iota(value.shape, 1)
    width = within.shape[1]
    even = lax.axis_index("param") % 2 == 0
    before = jnp.where(even, across[:, width - 1 :], within[:, width - 1 :])
    after = jnp.where(even, within[:, :1], across[:, :1])
    left = jnp.where(lane == 0, before, pltpu.roll(value, 1, 1))
    right = jnp.where(lane == cols - 1, after, pltpu.roll(value, cols - 1, 1))
    value = (0.5 * value + 0.25 * (left + right)) * scale[...]
    out[...] = value[: times * group].reshape(times, group, cols)


def rotate(value, axis, shift):
    size = lax.axis_size(axis)
    return lax.ppermute(value, axis, [(i, (i + shift) % size) for i in range(size)])


def steps(series, kernel, prior_spectrum, prior_scale):
    freqs, senss, params = (lax.axis_size(a) for a in ("freq", "sens", "param"))
    probes, sens_dev, times = series.shape
    bins, cols = kernel.shape[1], kernel.shape[3]
    group = probes // senss
    block = 2 * bins * group
    rows = -(-times * group // 8) * 8
    shape = jax.ShapeDtypeStruct
    own_series = series.transpose(2, 0, 1).reshape(times * probes, sens_dev)
    pieces = [own_series] + [rotate(own_series, "freq", -j) for j in range(1, freqs)]
    *tables, spread = call(
        functools.partial(prepare_body, (bins, times, probes, group, freqs, senss)),
        [shape((senss * block, times * probes), BF)] * (2 * freqs)
        + [shape((sens_dev, sens_dev * bins), BF)],
        flops=PREP,
    )
    operator = kernel.transpose(0, 2, 1, 3).reshape(2 * sens_dev * bins, cols)
    edge = cols * OUTER // 16
    blocks = lambda width: [shape((block, width), BF if i else F32) for i in range(senss)]
    lhs_re, lhs_im, *outer = call(
        functools.partial(contract_body, bins, senss, freqs),
        [shape((senss * block, sens_dev * bins), BF)] * 2 + blocks(2 * edge),
        *tables, *pieces, spread, operator,
    )
    inner = call(inner_body, blocks(cols - 2 * edge), lhs_re, lhs_im, operator)
    inverse = call(
        functools.partial(inverse_body, (bins, times, group, freqs, rows)),
        shape((freqs * rows, block), F32),
        prior_spectrum.reshape(1, bins), outer[0],
    )
    order = sorted(range(1, senss), key=lambda d: -min(d, senss - d))
    outer = [outer[0]] + [rotate(outer[d], "sens", d) for d in order]
    inner = [inner[0]] + [rotate(inner[d], "sens", d) for d in order]
    images = lambda width: [shape((rows, width), BF if i else F32) for i in range(freqs)]
    as_image = functools.partial(image_body, rows)
    outer = call(as_image, images(2 * edge), inverse, *outer)
    outer = [outer[0]] + [rotate(outer[j], "freq", j) for j in range(1, freqs)]
    inner = call(as_image, images(cols - 2 * edge), inverse, *inner)
    inner = [inner[0]] + [rotate(inner[j], "freq", j) for j in range(1, freqs)]
    scale = prior_scale.reshape(1, cols)
    lanes = min(128, edge)
    swaps = list(call(
        functools.partial(edge_body, lanes), [shape((rows, lanes), F32)] * 2, scale, *outer)
    )
    for i in (0, 1):
        pairs = [(a, a + 1) for a in range(i, params - 1, 2)]
        swaps[i] = lax.ppermute(swaps[i], "param", pairs + [(b, a) for a, b in pairs])
    return call(
        functools.partial(smooth_body, freqs),
        shape((times, group, cols), F32),
        scale, *swaps, *outer, *inner,
    )


def solution(mesh):
    placed = (P(None, "sens", "freq"), P(None, "freq", "sens", "param"), P("freq"), P("param"))
    return jax.shard_map(
        steps, mesh=mesh, in_specs=placed, out_specs=P("freq", "sens", "param"), check_vma=False
    )
```

```python
import functools
import math

import jax
import jax.numpy as jnp
from jax import lax
from jax.experimental import pallas as pl
from jax.experimental.pallas import tpu as pltpu
from jax.sharding import PartitionSpec as P


LEN = 840
OUTER = 4
PREP = 10**10
BF = jnp.bfloat16
F32 = jnp.float32


def vmem():
    return pl.BlockSpec(memory_space=pltpu.VMEM)


def call(body, out_shape, *args, flops=0, limit=4 << 20):
    moved = sum(a.size * a.dtype.itemsize for a in [*args, *jax.tree.leaves(out_shape)])
    return pl.pallas_call(
        body,
        in_specs=[vmem()] * len(args),
        out_specs=jax.tree.map(lambda _: vmem(), out_shape),
        out_shape=out_shape,
        compiler_params=pltpu.CompilerParams(vmem_limit_bytes=limit),
        cost_estimate=pl.CostEstimate(flops=flops, transcendentals=0, bytes_accessed=moved),
    )(*args)


def split_index(flat, sizes):
    out = []
    for size in reversed(sizes):
        out.append(flat % size)
        flat = flat // size
    return out[::-1]


def iota(shape, dim):
    return lax.broadcasted_iota(jnp.int32, shape, dim)


def onehot(shape, hit):
    return jnp.where(hit, jnp.ones(shape, F32), jnp.zeros(shape, F32)).astype(BF)


def dot(a, b, precision=None):
    return jnp.dot(a, b, precision=precision, preferred_element_type=F32)


def wave(product, part):
    angle = ((product + part * (LEN // 4)) % LEN).astype(F32) * (2.0 * math.pi / LEN)
    return jnp.cos(angle)


def prepare_body(dims, *refs):
    bins, times, probes, group, freqs, senss = dims
    freq, sens = lax.axis_index("freq"), lax.axis_index("sens")
    tables, spread = refs[: 2 * freqs], refs[2 * freqs]
    small = (2 * bins, times)
    part, bin_at = split_index(iota(small, 0), (2, bins))
    tall = (senss * 2 * bins * group, 2 * bins)
    up = onehot(tall, iota(tall, 0) // group % (2 * bins) == iota(tall, 1))
    flat = (times, times * probes)
    out = onehot(flat, iota(flat, 1) // probes == iota(flat, 0))
    full = (tall[0], flat[1])
    shift = iota(full, 0) // (2 * bins * group)
    probe = (sens + shift) % senss * group + iota(full, 0) % group
    hit = iota(full, 1) % probes == probe
    for j in range(freqs):
        time = iota(small, 1) + (freq + j) % freqs * times
        value = wave((freq * bins + bin_at) * time, part) * (1.0 / math.sqrt(times * freqs))
        high = value.astype(BF)
        low = (value - high.astype(F32)).astype(BF)
        for i, piece in enumerate((high, low)):
            wide = dot(dot(up, piece).astype(BF), out)
            tables[2 * j + i][...] = jnp.where(hit, wide, 0.0).astype(BF)
    spread[...] = onehot(spread.shape, iota(spread.shape, 1) // bins == iota(spread.shape, 0))


def inverse_body(dims, weights, after, inverse):
    bins, times, group, freqs, rows = dims
    freq = lax.axis_index("freq")
    shape = inverse.shape
    shift, row = split_index(iota(shape, 0), (freqs, rows))
    part, bin_at, inner = split_index(iota(shape, 1), (2, bins, group))
    time = row // group + (freq + shift) % freqs * times
    value = wave((freq * bins + bin_at) * time, part)
    pick = (bins, shape[1])
    chosen = jnp.where(iota(pick, 1) // group % bins == iota(pick, 0), 1.0, 0.0)
    weight = dot(weights[...], chosen, lax.Precision.HIGHEST) * (1.0 / math.sqrt(bins * freqs))
    hit = (row % group == inner) & (row < times * group)
    inverse[...] = jnp.where(hit, value * weight[:1], 0.0)


def contract_body(bins, blocks, pieces, *refs):
    tables = refs[: 2 * pieces]
    series = refs[2 * pieces : 3 * pieces]
    spread, operator = refs[3 * pieces : 3 * pieces + 2]
    lhs_re, lhs_im = refs[3 * pieces + 2 : 3 * pieces + 4]
    spec = None
    for i in range(2 * pieces):
        term = dot(tables[i][...], series[i // 2][...])
        spec = term if spec is None else spec + term
    rows = spec.shape[0]
    block = rows // blocks
    half = block // 2
    group = half // bins
    wide = dot(spec.astype(BF), spread[...])
    keep = iota(wide.shape, 0) // group % bins == iota(wide.shape, 1) % bins
    wide = jnp.where(keep, wide, 0.0).astype(BF)
    lhs_re[...] = wide
    for i in range(blocks):
        lhs_im[i * block : i * block + half, :] = wide[i * block + half : (i + 1) * block]
        lhs_im[i * block + half : (i + 1) * block, :] = -wide[i * block : i * block + half]
    outer_body(lhs_re, lhs_im, operator, *refs[3 * pieces + 4 :])


def product(lhs_re, lhs_im, operator, first, count):
    inner = operator.shape[0] // 2
    at = pl.ds(first, count)
    return dot(lhs_re[...], operator[:inner, at]) + dot(lhs_im[...], operator[inner:, at])


def outer_body(lhs_re, lhs_im, operator, *outs):
    cols, edge = operator.shape[1], outs[0].shape[1] // 2
    block = lhs_re.shape[0] // len(outs)
    for at, first in ((0, 0), (edge, cols - edge)):
        total = product(lhs_re, lhs_im, operator, first, edge)
        for i, out in enumerate(outs):
            out[:, at : at + edge] = total[i * block : (i + 1) * block].astype(out.dtype)


def inner_body(lhs_re, lhs_im, operator, *outs):
    width = outs[0].shape[1]
    block = lhs_re.shape[0] // len(outs)
    total = product(lhs_re, lhs_im, operator, (operator.shape[1] - width) // 2, width)
    for i, out in enumerate(outs):
        out[...] = total[i * block : (i + 1) * block].astype(out.dtype)


def image_body(rows, *refs):
    table, own = refs[:2]
    count = table.shape[0] // rows
    outs = refs[len(refs) - count :]
    total = own[...]
    for other in refs[2 : len(refs) - count]:
        total = total + other[...].astype(F32)
    image = dot(table[...], total, lax.Precision.HIGHEST)
    for i, out in enumerate(outs):
        out[...] = image[i * rows : (i + 1) * rows].astype(out.dtype)


def edge_body(lanes, scale, *refs):
    within, across = refs[-2:]
    cols, width = scale.shape[1], refs[0].shape[1]

    def scaled(at, scale_at):
        total = None
        for ref in refs[:-2]:
            term = ref[:, at : at + lanes].astype(F32)
            total = term if total is None else total + term
        return total * scale[:, scale_at : scale_at + lanes]

    first, last = scaled(0, 0), scaled(width - lanes, cols - lanes)
    even = lax.axis_index("param") % 2 == 0
    within[...] = jnp.where(even, last, first)
    across[...] = jnp.where(even, first, last)


def smooth_body(count, scale, within, across, *refs):
    out = refs[-1]

    def total(parts):
        value = parts[0][...]
        for ref in parts[1:]:
            value = value + ref[...].astype(F32)
        return value

    outer, inner = total(refs[:count]), total(refs[count:-1])
    times, group, cols = out.shape
    edge = outer.shape[1] // 2
    value = jnp.concatenate([outer[:, :edge], inner, outer[:, edge:]], axis=1)
    value = value * scale[...]
    lane = iota(value.shape, 1)
    width = within.shape[1]
    at, ends = lax.axis_index("param"), lax.axis_size("param") - 1
    even = at % 2 == 0
    before = jnp.where(even, across[:, width - 1 :], within[:, width - 1 :])
    after = jnp.where(even, within[:, :1], across[:, :1])
    before, after = jnp.where(at > 0, before, 0.0), jnp.where(at < ends, after, 0.0)
    left = jnp.where(lane == 0, before, pltpu.roll(value, 1, 1))
    right = jnp.where(lane == cols - 1, after, pltpu.roll(value, cols - 1, 1))
    value = (0.5 * value + 0.25 * (left + right)) * scale[...]
    out[...] = value[: times * group].reshape(times, group, cols)


def rotate(value, axis, shift):
    size = lax.axis_size(axis)
    return lax.ppermute(value, axis, [(i, (i + shift) % size) for i in range(size)])


def steps(series, kernel, prior_spectrum, prior_scale):
    freqs, senss, params = (lax.axis_size(a) for a in ("freq", "sens", "param"))
    probes, sens_dev, times = series.shape
    bins, cols = kernel.shape[1], kernel.shape[3]
    group = probes // senss
    block = 2 * bins * group
    rows = -(-times * group // 8) * 8
    shape = jax.ShapeDtypeStruct
    own_series = series.transpose(2, 0, 1).reshape(times * probes, sens_dev)
    pieces = [own_series] + [rotate(own_series, "freq", -j) for j in range(1, freqs)]
    *tables, spread = call(
        functools.partial(prepare_body, (bins, times, probes, group, freqs, senss)),
        [shape((senss * block, times * probes), BF)] * (2 * freqs)
        + [shape((sens_dev, sens_dev * bins), BF)],
        flops=PREP,
    )
    operator = kernel.transpose(0, 2, 1, 3).reshape(2 * sens_dev * bins, cols)
    edge = cols * OUTER // 16
    blocks = lambda width: [shape((block, width), BF if i else F32) for i in range(senss)]
    lhs_re, lhs_im, *outer = call(
        functools.partial(contract_body, bins, senss, freqs),
        [shape((senss * block, sens_dev * bins), BF)] * 2 + blocks(2 * edge),
        *tables, *pieces, spread, operator,
    )
    inner = call(inner_body, blocks(cols - 2 * edge), lhs_re, lhs_im, operator)
    inverse = call(
        functools.partial(inverse_body, (bins, times, group, freqs, rows)),
        shape((freqs * rows, block), F32),
        prior_spectrum.reshape(1, bins), outer[0],
    )
    order = sorted(range(1, senss), key=lambda d: -min(d, senss - d))
    outer = [outer[0]] + [rotate(outer[d], "sens", d) for d in order]
    inner = [inner[0]] + [rotate(inner[d], "sens", d) for d in order]
    images = lambda width: [shape((rows, width), BF if i else F32) for i in range(freqs)]
    as_image = functools.partial(image_body, rows)
    outer = call(as_image, images(2 * edge), inverse, *outer)
    outer = [outer[0]] + [rotate(outer[j], "freq", j) for j in range(1, freqs)]
    inner = call(as_image, images(cols - 2 * edge), inverse, *inner)
    inner = [inner[0]] + [rotate(inner[j], "freq", j) for j in range(1, freqs)]
    scale = prior_scale.reshape(1, cols)
    lanes = min(128, edge)
    swaps = list(call(
        functools.partial(edge_body, lanes), [shape((rows, lanes), F32)] * 2, scale, *outer)
    )
    for i in (0, 1):
        pairs = [(a, (a + 1) % params) for a in range(i, params // 2 * 2, 2)]
        swaps[i] = lax.ppermute(swaps[i], "param", pairs + [(b, a) for a, b in pairs])
    return call(
        functools.partial(smooth_body, freqs),
        shape((times, group, cols), F32),
        scale, *swaps, *outer, *inner,
    )


def solution(mesh):
    placed = (P(None, "sens", "freq"), P(None, "freq", "sens", "param"), P("freq"), P("param"))
    return jax.shard_map(
        steps, mesh=mesh, in_specs=placed, out_specs=P("freq", "sens", "param"), check_vma=False
    )
```

```python
import functools
import math

import jax
import jax.numpy as jnp
from jax import lax
from jax.experimental import pallas as pl
from jax.experimental.pallas import tpu as pltpu
from jax.sharding import PartitionSpec as P


LEN = 840
OUTER = 4
PREP = 10**10
BF = jnp.bfloat16
F32 = jnp.float32


def vmem():
    return pl.BlockSpec(memory_space=pltpu.VMEM)


def call(body, out_shape, *args, flops=0, limit=4 << 20):
    moved = sum(a.size * a.dtype.itemsize for a in [*args, *jax.tree.leaves(out_shape)])
    return pl.pallas_call(
        body,
        in_specs=[vmem()] * len(args),
        out_specs=jax.tree.map(lambda _: vmem(), out_shape),
        out_shape=out_shape,
        compiler_params=pltpu.CompilerParams(vmem_limit_bytes=limit),
        cost_estimate=pl.CostEstimate(flops=flops, transcendentals=0, bytes_accessed=moved),
    )(*args)


def split_index(flat, sizes):
    out = []
    for size in reversed(sizes):
        out.append(flat % size)
        flat = flat // size
    return out[::-1]


def iota(shape, dim):
    return lax.broadcasted_iota(jnp.int32, shape, dim)


def rows_of(count):
    return iota((count, 1), 0)


def cols_of(count):
    return iota((1, count), 1)


def onehot(hit):
    return jnp.where(hit, 1.0, 0.0).astype(BF)


def dot(a, b, precision=None):
    return jnp.dot(a, b, precision=precision, preferred_element_type=F32)


def wave(product, part):
    angle = ((product + part * (LEN // 4)) % LEN).astype(F32) * (2.0 * math.pi / LEN)
    return jnp.cos(angle)


def prepare_body(dims, *refs):
    bins, times, probes, group, freqs, senss = dims
    freq, sens = lax.axis_index("freq"), lax.axis_index("sens")
    tables, spread = refs[: 2 * freqs], refs[2 * freqs]
    part, bin_at = split_index(rows_of(2 * bins), (2, bins))
    tall, wide = senss * 2 * bins * group, times * probes
    up = onehot(rows_of(tall) // group % (2 * bins) == cols_of(2 * bins))
    out = onehot(cols_of(wide) // probes == rows_of(times))
    shift = rows_of(tall) // (2 * bins * group)
    probe = (sens + shift) % senss * group + rows_of(tall) % group
    hit = cols_of(wide) % probes == probe
    for j in range(freqs):
        time = cols_of(times) + (freq + j) % freqs * times
        value = wave((freq * bins + bin_at) * time, part) * (1.0 / math.sqrt(times * freqs))
        high = value.astype(BF)
        low = (value - high.astype(F32)).astype(BF)
        for i, piece in enumerate((high, low)):
            spaced = dot(dot(up, piece).astype(BF), out)
            tables[2 * j + i][...] = jnp.where(hit, spaced, 0.0).astype(BF)
    spread[...] = onehot(cols_of(spread.shape[1]) // bins == rows_of(spread.shape[0]))


def inverse_body(dims, weights, high, low):
    bins, times, group, freqs, rows = dims
    freq = lax.axis_index("freq")
    shift, row = split_index(rows_of(freqs * rows), (freqs, rows))
    part, bin_at, inner = split_index(cols_of(2 * bins * group), (2, bins, group))
    time = row // group + (freq + shift) % freqs * times
    value = wave((freq * bins + bin_at) * time, part)
    chosen = jnp.where(bin_at == rows_of(bins), 1.0, 0.0)
    weight = dot(weights[...], chosen, lax.Precision.HIGHEST) * (1.0 / math.sqrt(bins * freqs))
    hit = (row % group == inner) & (row < times * group)
    value = jnp.where(hit, value * weight[:1], 0.0)
    high[...] = value.astype(BF)
    low[...] = (value - high[...].astype(F32)).astype(BF)


def spectrum(tables, series, total=None):
    for i, table in enumerate(tables):
        term = dot(table[...], series[i // 2][...])
        total = term if total is None else total + term
    return total


def own_body(high, low, series, out):
    out[...] = spectrum((high, low), (series,))


def contract_body(bins, blocks, pieces, own, *refs):
    tables = refs[: 2 * pieces]
    series = refs[2 * pieces : 3 * pieces]
    spread, operator = refs[3 * pieces : 3 * pieces + 2]
    lhs_re, lhs_im = refs[3 * pieces + 2 : 3 * pieces + 4]
    spec = spectrum(tables, series, own[...])
    rows = spec.shape[0]
    block = rows // blocks
    half = block // 2
    group = half // bins
    wide = dot(spec.astype(BF), spread[...])
    keep = rows_of(rows) // group % bins == cols_of(wide.shape[1]) % bins
    wide = jnp.where(keep, wide, 0.0).astype(BF)
    lhs_re[...] = wide
    for i in range(blocks):
        lhs_im[i * block : i * block + half, :] = wide[i * block + half : (i + 1) * block]
        lhs_im[i * block + half : (i + 1) * block, :] = -wide[i * block : i * block + half]
    outer_body(lhs_re, lhs_im, operator, *refs[3 * pieces + 4 :])


def product(lhs_re, lhs_im, operator, first, count):
    inner = operator.shape[0] // 2
    at = pl.ds(first, count)
    return dot(lhs_re[...], operator[:inner, at]) + dot(lhs_im[...], operator[inner:, at])


def outer_body(lhs_re, lhs_im, operator, *outs):
    cols, edge = operator.shape[1], outs[0].shape[1] // 2
    block = lhs_re.shape[0] // len(outs)
    for at, first in ((0, 0), (edge, cols - edge)):
        total = product(lhs_re, lhs_im, operator, first, edge)
        for i, out in enumerate(outs):
            out[:, at : at + edge] = total[i * block : (i + 1) * block].astype(out.dtype)


def inner_body(lhs_re, lhs_im, operator, *outs):
    width = outs[0].shape[1]
    block = lhs_re.shape[0] // len(outs)
    total = product(lhs_re, lhs_im, operator, (operator.shape[1] - width) // 2, width)
    for i, out in enumerate(outs):
        out[...] = total[i * block : (i + 1) * block].astype(out.dtype)


def image_body(rows, high, low, own, *refs):
    count = high.shape[0] // rows
    outs = refs[len(refs) - count :]
    total = own[...]
    for other in refs[: len(refs) - count]:
        total = total + other[...].astype(F32)
    upper = total.astype(BF)
    lower = (total - upper.astype(F32)).astype(BF)
    image = dot(high[...], upper) + (dot(high[...], lower) + dot(low[...], upper))
    for i, out in enumerate(outs):
        out[...] = image[i * rows : (i + 1) * rows].astype(out.dtype)


def edge_body(scale, *refs):
    within, across = refs[-2:]
    cols, width = scale.shape[1], refs[0].shape[1]
    count = refs[0].shape[0]
    eye = rows_of(count) == cols_of(within.shape[1])

    def column(at, scale_at):
        total = None
        for ref in refs[:-2]:
            term = ref[:, at : at + 1].astype(F32)
            total = term if total is None else total + term
        total = total * scale[:, scale_at : scale_at + 1]
        return jnp.sum(jnp.where(eye, total, 0.0), axis=0, keepdims=True)

    first, last = column(0, 0), column(width - 1, cols - 1)
    even = lax.axis_index("param") % 2 == 0
    within[...] = jnp.broadcast_to(jnp.where(even, last, first), within.shape)
    across[...] = jnp.broadcast_to(jnp.where(even, first, last), across.shape)


def smooth_body(count, scale, within, across, *refs):
    out = refs[-1]

    def total(parts):
        value = parts[0][...]
        for ref in parts[1:]:
            value = value + ref[...].astype(F32)
        return value

    outer, inner = total(refs[:count]), total(refs[count:-1])
    times, group, cols = out.shape
    edge = outer.shape[1] // 2
    value = jnp.concatenate([outer[:, :edge], inner, outer[:, edge:]], axis=1)
    value = value * scale[...]
    lane = cols_of(cols)
    at, ends = lax.axis_index("param"), lax.axis_size("param") - 1
    eye = rows_of(value.shape[0]) == cols_of(within.shape[1])
    within, across = within[:1], across[:1]
    even = at % 2 == 0
    before = jnp.where(even & (at > 0), across, jnp.where(even, 0.0, within))
    after = jnp.where(even, within, jnp.where(at < ends, across, 0.0))
    before, after = (
        jnp.sum(jnp.where(eye, row, 0.0), axis=1, keepdims=True) for row in (before, after)
    )
    left = jnp.where(lane == 0, before, pltpu.roll(value, 1, 1))
    right = jnp.where(lane == cols - 1, after, pltpu.roll(value, cols - 1, 1))
    value = (0.5 * value + 0.25 * (left + right)) * scale[...]
    out[...] = value[: times * group].reshape(times, group, cols)


def rotate(value, axis, shift):
    size = lax.axis_size(axis)
    return lax.ppermute(value, axis, [(i, (i + shift) % size) for i in range(size)])


def steps(series, kernel, prior_spectrum, prior_scale):
    freqs, senss, params = (lax.axis_size(a) for a in ("freq", "sens", "param"))
    probes, sens_dev, times = series.shape
    bins, cols = kernel.shape[1], kernel.shape[3]
    group = probes // senss
    block = 2 * bins * group
    rows = -(-times * group // 8) * 8
    shape = jax.ShapeDtypeStruct
    own_series = series.transpose(2, 0, 1).reshape(times * probes, sens_dev)
    pieces = [own_series] + [rotate(own_series, "freq", -j) for j in range(1, freqs)]
    *tables, spread = call(
        functools.partial(prepare_body, (bins, times, probes, group, freqs, senss)),
        [shape((senss * block, times * probes), BF)] * (2 * freqs)
        + [shape((sens_dev, sens_dev * bins), BF)],
        flops=PREP,
    )
    operator = kernel.transpose(0, 2, 1, 3).reshape(2 * sens_dev * bins, cols)
    edge = cols * OUTER // 16
    blocks = lambda width: [shape((block, width), BF if i else F32) for i in range(senss)]
    own = call(own_body, shape((senss * block, sens_dev), F32), *tables[:2], own_series)
    lhs_re, lhs_im, *outer = call(
        functools.partial(contract_body, bins, senss, freqs - 1),
        [shape((senss * block, sens_dev * bins), BF)] * 2 + blocks(2 * edge),
        own, *tables[2:], *pieces[1:], spread, operator,
    )
    inner = call(inner_body, blocks(cols - 2 * edge), lhs_re, lhs_im, operator)
    inverse = call(
        functools.partial(inverse_body, (bins, times, group, freqs, rows)),
        [shape((freqs * rows, block), BF)] * 2,
        prior_spectrum.reshape(1, bins),
    )
    order = sorted(range(1, senss), key=lambda d: -min(d, senss - d))
    outer = [outer[0]] + [rotate(outer[d], "sens", d) for d in order]
    inner = [inner[0]] + [rotate(inner[d], "sens", d) for d in order]
    images = lambda width: [shape((rows, width), BF if i else F32) for i in range(freqs)]
    as_image = functools.partial(image_body, rows)
    outer = call(as_image, images(2 * edge), *inverse, *outer)
    outer = [outer[0]] + [rotate(outer[j], "freq", j) for j in range(1, freqs)]
    inner = call(as_image, images(cols - 2 * edge), *inverse, *inner)
    inner = [inner[0]] + [rotate(inner[j], "freq", j) for j in range(1, freqs)]
    scale = prior_scale.reshape(1, cols)
    row = shape((8, -(-rows // 128) * 128), F32)
    swaps = list(call(edge_body, [row] * 2, scale, *outer))
    for i in (0, 1):
        pairs = [(a, (a + 1) % params) for a in range(i, params // 2 * 2, 2)]
        swaps[i] = lax.ppermute(swaps[i], "param", pairs + [(b, a) for a, b in pairs])
    return call(
        functools.partial(smooth_body, freqs),
        shape((times, group, cols), F32),
        scale, *swaps, *outer, *inner,
    )


def solution(mesh):
    placed = (P(None, "sens", "freq"), P(None, "freq", "sens", "param"), P("freq"), P("param"))
    return jax.shard_map(
        steps, mesh=mesh, in_specs=placed, out_specs=P("freq", "sens", "param"), check_vma=False
    )
```

```python
import functools
import math

import jax
import jax.numpy as jnp
from jax import lax
from jax.experimental import pallas as pl
from jax.experimental.pallas import tpu as pltpu
from jax.sharding import PartitionSpec as P


LEN = 840
OUTER = 4
PREP = 10**10
EARLY = 1
BF = jnp.bfloat16
F32 = jnp.float32


def vmem():
    return pl.BlockSpec(memory_space=pltpu.VMEM)


def call(body, out_shape, *args, flops=0, aliases={}, limit=4 << 20):
    moved = sum(a.size * a.dtype.itemsize for a in [*args, *jax.tree.leaves(out_shape)])
    return pl.pallas_call(
        body,
        in_specs=[vmem()] * len(args),
        out_specs=jax.tree.map(lambda _: vmem(), out_shape),
        out_shape=out_shape,
        input_output_aliases=aliases,
        compiler_params=pltpu.CompilerParams(vmem_limit_bytes=limit),
        cost_estimate=pl.CostEstimate(flops=flops, transcendentals=0, bytes_accessed=moved),
    )(*args)


def split_index(flat, sizes):
    out = []
    for size in reversed(sizes):
        out.append(flat % size)
        flat = flat // size
    return out[::-1]


def iota(shape, dim):
    return lax.broadcasted_iota(jnp.int32, shape, dim)


def rows_of(count):
    return iota((count, 1), 0)


def cols_of(count):
    return iota((1, count), 1)


def onehot(hit):
    return jnp.where(hit, 1.0, 0.0).astype(BF)


def dot(a, b, precision=None):
    return jnp.dot(a, b, precision=precision, preferred_element_type=F32)


def wave(product, part):
    angle = ((product + part * (LEN // 4)) % LEN).astype(F32) * (2.0 * math.pi / LEN)
    return jnp.cos(angle)


def prepare_body(dims, *refs):
    bins, times, probes, group, freqs, senss = dims
    freq, sens = lax.axis_index("freq"), lax.axis_index("sens")
    tables, spread = refs[: 2 * freqs], refs[2 * freqs]
    part, bin_at = split_index(rows_of(2 * bins), (2, bins))
    tall, wide = senss * 2 * bins * group, times * probes
    up = onehot(rows_of(tall) // group % (2 * bins) == cols_of(2 * bins))
    out = onehot(cols_of(wide) // probes == rows_of(times))
    shift = rows_of(tall) // (2 * bins * group)
    probe = (sens + shift) % senss * group + rows_of(tall) % group
    hit = cols_of(wide) % probes == probe
    for j in range(freqs):
        time = cols_of(times) + (freq + j) % freqs * times
        value = wave((freq * bins + bin_at) * time, part) * (1.0 / math.sqrt(times * freqs))
        high = value.astype(BF)
        low = (value - high.astype(F32)).astype(BF)
        for i, piece in enumerate((high, low)):
            spaced = dot(dot(up, piece).astype(BF), out)
            tables[2 * j + i][...] = jnp.where(hit, spaced, 0.0).astype(BF)
    spread[...] = onehot(cols_of(spread.shape[1]) // bins == rows_of(spread.shape[0]))


def inverse_body(dims, weights, high, low):
    bins, times, group, freqs, rows = dims
    freq = lax.axis_index("freq")
    shift, row = split_index(rows_of(freqs * rows), (freqs, rows))
    part, bin_at, inner = split_index(cols_of(2 * bins * group), (2, bins, group))
    time = row // group + (freq + shift) % freqs * times
    value = wave((freq * bins + bin_at) * time, part)
    chosen = jnp.where(bin_at == rows_of(bins), 1.0, 0.0)
    weight = dot(weights[...], chosen, lax.Precision.HIGHEST) * (1.0 / math.sqrt(bins * freqs))
    hit = (row % group == inner) & (row < times * group)
    value = jnp.where(hit, value * weight[:1], 0.0)
    high[...] = value.astype(BF)
    low[...] = (value - high[...].astype(F32)).astype(BF)


def spectrum(tables, series, total=None):
    for i, table in enumerate(tables):
        term = dot(table[...], series[i // 2][...])
        total = term if total is None else total + term
    return total


def own_body(high, low, series, out):
    out[...] = spectrum((high, low), (series,))


def contract_body(bins, blocks, pieces, own, *refs):
    tables = refs[: 2 * pieces]
    series = refs[2 * pieces : 3 * pieces]
    spread, operator = refs[3 * pieces : 3 * pieces + 2]
    lhs_re, lhs_im = refs[3 * pieces + 2 : 3 * pieces + 4]
    spec = spectrum(tables, series, own[...])
    rows = spec.shape[0]
    block = rows // blocks
    half = block // 2
    group = half // bins
    wide = dot(spec.astype(BF), spread[...])
    keep = rows_of(rows) // group % bins == cols_of(wide.shape[1]) % bins
    wide = jnp.where(keep, wide, 0.0).astype(BF)
    lhs_re[...] = wide
    for i in range(blocks):
        lhs_im[i * block : i * block + half, :] = wide[i * block + half : (i + 1) * block]
        lhs_im[i * block + half : (i + 1) * block, :] = -wide[i * block : i * block + half]
    outer_body(lhs_re, lhs_im, operator, *refs[3 * pieces + 4 :])


def product(lhs_re, lhs_im, operator, first, count):
    inner = operator.shape[0] // 2
    at = pl.ds(first, count)
    return dot(lhs_re[...], operator[:inner, at]) + dot(lhs_im[...], operator[inner:, at])


def outer_body(lhs_re, lhs_im, operator, *outs):
    cols, edge = operator.shape[1], outs[0].shape[1] // 2
    block = lhs_re.shape[0] // len(outs)
    for at, first in ((0, 0), (edge, cols - edge)):
        total = product(lhs_re, lhs_im, operator, first, edge)
        for i, out in enumerate(outs):
            out[:, at : at + edge] = total[i * block : (i + 1) * block].astype(out.dtype)


def inner_body(turn, blocks, lhs_re, lhs_im, operator, *refs):
    @pl.when(lax.axis_index("param") % 2 == turn)
    def _():
        inner_product(lhs_re, lhs_im, operator, *refs[-blocks:])


def inner_product(lhs_re, lhs_im, operator, *outs):
    width = outs[0].shape[1]
    block = lhs_re.shape[0] // len(outs)
    total = product(lhs_re, lhs_im, operator, (operator.shape[1] - width) // 2, width)
    for i, out in enumerate(outs):
        out[...] = total[i * block : (i + 1) * block].astype(out.dtype)


def image_body(rows, high, low, own, *refs):
    count = high.shape[0] // rows
    outs = refs[len(refs) - count :]
    total = own[...]
    for other in refs[: len(refs) - count]:
        total = total + other[...].astype(F32)
    upper = total.astype(BF)
    lower = (total - upper.astype(F32)).astype(BF)
    image = dot(high[...], upper) + (dot(high[...], lower) + dot(low[...], upper))
    for i, out in enumerate(outs):
        out[...] = image[i * rows : (i + 1) * rows].astype(out.dtype)


def edge_body(scale, *refs):
    within, across = refs[-2:]
    cols, width = scale.shape[1], refs[0].shape[1]
    count = refs[0].shape[0]
    eye = rows_of(count) == cols_of(within.shape[1])

    def column(at, scale_at):
        total = None
        for ref in refs[:-2]:
            term = ref[:, at : at + 1].astype(F32)
            total = term if total is None else total + term
        total = total * scale[:, scale_at : scale_at + 1]
        return jnp.sum(jnp.where(eye, total, 0.0), axis=0, keepdims=True)

    first, last = column(0, 0), column(width - 1, cols - 1)
    even = lax.axis_index("param") % 2 == 0
    within[...] = jnp.broadcast_to(jnp.where(even, last, first), within.shape)
    across[...] = jnp.broadcast_to(jnp.where(even, first, last), across.shape)


def smooth_body(count, scale, within, across, *refs):
    out = refs[-1]

    def total(parts):
        value = parts[0][...]
        for ref in parts[1:]:
            value = value + ref[...].astype(F32)
        return value

    outer, inner = total(refs[:count]), total(refs[count:-1])
    times, group, cols = out.shape
    edge = outer.shape[1] // 2
    value = jnp.concatenate([outer[:, :edge], inner, outer[:, edge:]], axis=1)
    value = value * scale[...]
    lane = cols_of(cols)
    at, ends = lax.axis_index("param"), lax.axis_size("param") - 1
    eye = rows_of(value.shape[0]) == cols_of(within.shape[1])
    within, across = within[:1], across[:1]
    even = at % 2 == 0
    before = jnp.where(even & (at > 0), across, jnp.where(even, 0.0, within))
    after = jnp.where(even, within, jnp.where(at < ends, across, 0.0))
    before, after = (
        jnp.sum(jnp.where(eye, row, 0.0), axis=1, keepdims=True) for row in (before, after)
    )
    left = jnp.where(lane == 0, before, pltpu.roll(value, 1, 1))
    right = jnp.where(lane == cols - 1, after, pltpu.roll(value, cols - 1, 1))
    value = (0.5 * value + 0.25 * (left + right)) * scale[...]
    out[...] = value[: times * group].reshape(times, group, cols)


def rotate(value, axis, shift):
    size = lax.axis_size(axis)
    return lax.ppermute(value, axis, [(i, (i + shift) % size) for i in range(size)])


def steps(series, kernel, prior_spectrum, prior_scale):
    freqs, senss, params = (lax.axis_size(a) for a in ("freq", "sens", "param"))
    probes, sens_dev, times = series.shape
    bins, cols = kernel.shape[1], kernel.shape[3]
    group = probes // senss
    block = 2 * bins * group
    rows = -(-times * group // 8) * 8
    shape = jax.ShapeDtypeStruct
    own_series = series.transpose(2, 0, 1).reshape(times * probes, sens_dev)
    pieces = [own_series] + [rotate(own_series, "freq", -j) for j in range(1, freqs)]
    *tables, spread = call(
        functools.partial(prepare_body, (bins, times, probes, group, freqs, senss)),
        [shape((senss * block, times * probes), BF)] * (2 * freqs)
        + [shape((sens_dev, sens_dev * bins), BF)],
        flops=PREP,
    )
    operator = kernel.transpose(0, 2, 1, 3).reshape(2 * sens_dev * bins, cols)
    edge = cols * OUTER // 16
    blocks = lambda width: [shape((block, width), BF if i else F32) for i in range(senss)]
    own = call(own_body, shape((senss * block, sens_dev), F32), *tables[:2], own_series)
    lhs_re, lhs_im, *outer = call(
        functools.partial(contract_body, bins, senss, freqs - 1),
        [shape((senss * block, sens_dev * bins), BF)] * 2 + blocks(2 * edge),
        own, *tables[2:], *pieces[1:], spread, operator,
    )
    factors = (lhs_re, lhs_im, operator)
    inner = blocks(cols - 2 * edge)
    early = call(functools.partial(inner_body, EARLY, senss), inner, *factors)
    inner = call(
        functools.partial(inner_body, 1 - EARLY, senss),
        inner, *factors, *early,
        aliases={len(factors) + i: i for i in range(senss)},
    )
    inverse = call(
        functools.partial(inverse_body, (bins, times, group, freqs, rows)),
        [shape((freqs * rows, block), BF)] * 2,
        prior_spectrum.reshape(1, bins),
    )
    order = sorted(range(1, senss), key=lambda d: -min(d, senss - d))
    outer = [outer[0]] + [rotate(outer[d], "sens", d) for d in order]
    inner = [inner[0]] + [rotate(inner[d], "sens", d) for d in order]
    images = lambda width: [shape((rows, width), BF if i else F32) for i in range(freqs)]
    as_image = functools.partial(image_body, rows)
    outer = call(as_image, images(2 * edge), *inverse, *outer)
    outer = [outer[0]] + [rotate(outer[j], "freq", j) for j in range(1, freqs)]
    inner = call(as_image, images(cols - 2 * edge), *inverse, *inner)
    inner = [inner[0]] + [rotate(inner[j], "freq", j) for j in range(1, freqs)]
    scale = prior_scale.reshape(1, cols)
    row = shape((8, -(-rows // 128) * 128), F32)
    swaps = list(call(edge_body, [row] * 2, scale, *outer))
    for i in (0, 1):
        pairs = [(a, (a + 1) % params) for a in range(i, params // 2 * 2, 2)]
        swaps[i] = lax.ppermute(swaps[i], "param", pairs + [(b, a) for a, b in pairs])
    return call(
        functools.partial(smooth_body, freqs),
        shape((times, group, cols), F32),
        scale, *swaps, *outer, *inner,
    )


def solution(mesh):
    placed = (P(None, "sens", "freq"), P(None, "freq", "sens", "param"), P("freq"), P("param"))
    return jax.shard_map(
        steps, mesh=mesh, in_specs=placed, out_specs=P("freq", "sens", "param"), check_vma=False
    )
```
